32 devices in a mesh: group: 4 (over z), seq: 4 (over y, core), mp: 2 (over x).
Axes of the slice: x: 2, y: 2, z: 4, core: 2. Of those that a mesh axis runs over, the one named last changes fastest.
Arguments:
- patches: bfloat16 [8192, 640], P(('group', 'seq')), may hold values from -6 to 6
- w_merge1: bfloat16 [4, 640, 2560], P(None, 'seq', 'mp'), may hold values from -0.125 to 0.125
- w_merge2: bfloat16 [2560, 4096], P('mp', 'seq'), may hold values from -0.125 to 0.125
- w_query: bfloat16 [4096, 4096], P('seq', 'mp'), may hold values from -0.09375 to 0.09375
- w_keyval: bfloat16 [4096, 2, 1024], P('seq', None, 'mp'), may hold values from -0.09375 to 0.09375
- attn_grad: bfloat16 [2048, 4096], P(('group', 'seq'), 'mp'), may hold values from -6 to 6
- sample_ids: int32 [4, 512], P('group'), may hold values from 0 to 7, never falling along the last dimension, each value on 1 to 384 neighbouring positions
Outputs:
- patch_grad: bfloat16 [8192, 640], P(('group', 'seq', 'mp'))
The draws below stay inside these ranges and needn't reach their ends.
Inputs may be any that keep to these rules, and one draw needn't show every extreme that they name: `sample_ids`: in each sequence never falls; every sample spans 1 to 384 tokens.
All inputs are finite; a program needn't handle non-finite values.
Results may differ from the reference program's by a relative error of at most 0.035.
Values may be sent and summed in bfloat16 or wider, within the bound.
No kernel may reach another device: no remote copies, remote signals or barrier semaphores. Data moves between devices by JAX's collectives and lax.ppermute only.
A program may use at most 128 MiB of HBM per device.

```python
import math
import jax
import jax.numpy as jnp
import numpy as np
from jax import lax

V = 640
H = 2560
D = 4096
HEADS = 32
KV_HEADS = 8
HEAD = 128
TOK_SEQ = 128
SAMPLES = 8
RUN = 512
TOKENS = 2048
PATCHES = 8192
N_GROUP = 4
N_SEQ = 4
N_MP = 2


def block_scale(key, dims, split, least, high):
    factor_of = 1.0
    for position, blocks in split:
        heights = jax.random.uniform(jax.random.fold_in(jax.random.fold_in(key, 6), position), (blocks,), jnp.float32, least / len(split), high / len(split))
        factor_of = factor_of * jnp.repeat(jnp.exp(heights), dims[position] // blocks).reshape((-1,) + (1,) * (len(dims) - 1 - position))
    return factor_of


def length_profile(number_of, total, reach, lean):
    weights = [(1 << 20) // math.isqrt(standing ** lean) + 1 for standing in range(2, number_of + 1)]
    spare, given = total - reach - (number_of - 1), [1] * (number_of - 1)
    while spare > 0:
        candidates = [i for i in range(number_of - 1) if given[i] < reach]
        mass, remaining = sum([weights[i] for i in candidates]), spare
        for i in candidates:
            more = min(reach - given[i], max(1, remaining * weights[i] // mass), spare)
            given[i] = given[i] + more
            spare = spare - more
    return np.array([reach] + given)


def uneven_parts(stream_key, count, total, most, skew):
    if count == 2:
        one = jax.random.randint(stream_key, (), max(1, total - most), min(most, total - 1) + 1)
        return jnp.stack([one, total - one])
    sizes = jnp.asarray(length_profile(count, total, most, skew), jnp.int32)
    pairs = (count - 1) // 2
    donor, receiver = sizes[1:1 + 2 * pairs:2], sizes[2:2 + 2 * pairs:2]
    margin = jnp.minimum(donor - 1, most - receiver)
    moved = jax.random.randint(jax.random.fold_in(stream_key, 1), (pairs,), 0, 1 << 20) % (margin + 1)
    sizes = sizes.at[1:1 + 2 * pairs:2].set(donor - moved).at[2:2 + 2 * pairs:2].set(receiver + moved)
    return sizes[jax.random.permutation(jax.random.fold_in(stream_key, 2), count)]


def bell_draw(key, extent, deviation, limit, cuts=(), kind=jnp.bfloat16):
    gain = block_scale(key, extent, cuts, -0.22, 0.18) if cuts else 1.0
    result = jax.random.normal(key, extent, jnp.float32) * deviation * gain
    return jnp.minimum(jnp.maximum(result, -limit), limit).astype(kind)


def setup_inputs(seed: int = 0) -> dict:
    streams_of = jax.random.split(jax.random.key(seed), 8)
    patches = bell_draw(streams_of[0], (PATCHES, V), 1.0, 6.0, ((0, 16),))
    w_merge1 = bell_draw(streams_of[1], (4, V, H), (4 * V) ** -0.5, 0.125, ((1, 4), (2, 2)))
    w_merge2 = bell_draw(streams_of[2], (H, D), H ** -0.5, 0.125, ((0, 2), (1, 4)))
    w_query = bell_draw(streams_of[3], (D, HEADS * HEAD), D ** -0.5, 0.09375, ((0, 4), (1, 2)))
    w_keyval = bell_draw(streams_of[4], (D, 2, KV_HEADS * HEAD), D ** -0.5, 0.09375, ((0, 4), (2, 2)))
    attn_grad = bell_draw(streams_of[5], (TOKENS, HEADS * HEAD), 1.0, 6.0, ((0, 16), (1, 2)))
    sample_ids = jax.vmap(lambda own: jnp.searchsorted(jnp.cumsum(uneven_parts(own, SAMPLES, RUN, TOK_SEQ * N_SEQ // 2 + TOK_SEQ, 1)), jnp.arange(RUN), side="right"))(jax.random.split(streams_of[6], N_GROUP)).reshape((N_GROUP, RUN)).astype(jnp.int32)
    return {"patches": patches, "w_merge1": w_merge1, "w_merge2": w_merge2, "w_query": w_query, "w_keyval": w_keyval, "attn_grad": attn_grad, "sample_ids": sample_ids}


EPSILON = 1e-06
NEGATIVE = 1e+30

def gelu_grad(inputs):
    normal_cdf = 0.5 * (1.0 + lax.erf(inputs * 0.7071067811865476))
    normal_pdf = jnp.exp(-0.5 * inputs * inputs) * 0.3989422804014327
    return normal_cdf + inputs * normal_pdf

def block_sum(x_blocks, w_blocks):

    def advance(running, operands):
        product = jnp.dot(operands[0], operands[1], preferred_element_type=jnp.float32)
        rounded = lax.optimization_barrier(product.astype(jnp.bfloat16))
        return (running + rounded.astype(jnp.float32), None)
    initial = jnp.zeros((x_blocks.shape[1], w_blocks.shape[2]), jnp.float32)
    running, _ = lax.scan(advance, initial, (x_blocks, w_blocks))
    return running

def split_rows(inputs, blocks):
    return jnp.transpose(inputs.reshape(inputs.shape[0], blocks, inputs.shape[1] // blocks), (1, 0, 2))

def reference(patches, w_merge1, w_merge2, w_query, w_keyval, attn_grad, sample_ids):
    tokens = patches.shape[0] // 4
    run_len = tokens // N_GROUP
    kv_width = KV_HEADS * HEAD
    q_width = HEADS * HEAD
    per_kv = HEADS // KV_HEADS
    score_scale = HEAD ** (-0.5)
    values = patches.astype(jnp.float32)
    row_mean = lax.optimization_barrier(jnp.mean(values, -1, keepdims=True))
    ln_scale = lax.rsqrt(lax.optimization_barrier(jnp.mean(values * values, -1, keepdims=True)) - row_mean * row_mean + EPSILON)
    normed = (values - row_mean) * ln_scale
    merge_in = normed.astype(jnp.bfloat16).reshape(tokens, 4 * V)
    hidden_pre = jnp.dot(merge_in, w_merge1.reshape(4 * V, H), preferred_element_type=jnp.float32)
    hidden = jax.nn.gelu(hidden_pre, approximate=False).astype(jnp.bfloat16)
    merged = block_sum(split_rows(hidden, N_MP), w_merge2.reshape(N_MP, H // N_MP, D)).astype(jnp.bfloat16)
    merged_f = merged.astype(jnp.float32)
    rms_scale = lax.rsqrt(lax.optimization_barrier(jnp.mean(merged_f * merged_f, -1, keepdims=True)) + EPSILON)
    normed_tok = merged_f * rms_scale
    normed_bf = normed_tok.astype(jnp.bfloat16)
    queries = jnp.dot(normed_bf, w_query, preferred_element_type=jnp.float32).astype(jnp.bfloat16)
    keyval = jnp.dot(normed_bf, w_keyval.reshape(D, 2 * kv_width), preferred_element_type=jnp.float32).astype(jnp.bfloat16)

    def to_items(array, tail):
        shaped = array.reshape((N_GROUP, run_len, KV_HEADS) + tail)
        return jnp.moveaxis(shaped, 2, 1).reshape((N_GROUP * KV_HEADS, run_len) + tail)

    def from_items(array, tail, width):
        shaped = array.reshape((N_GROUP, KV_HEADS, run_len) + tail)
        return jnp.moveaxis(shaped, 1, 2).reshape(tokens, width)
    item_queries = to_items(queries, (per_kv, HEAD))
    item_keys = to_items(keyval[:, :kv_width], (HEAD,))
    item_values = to_items(keyval[:, kv_width:], (HEAD,))
    item_grads = to_items(attn_grad, (per_kv, HEAD))
    item_ids = jnp.repeat(sample_ids, KV_HEADS, axis=0)
    positions = jnp.arange(run_len, dtype=jnp.int32)

    def head_grads(operands):
        query_f = operands[0].astype(jnp.float32)
        key_f = operands[1].astype(jnp.float32)
        value_f = operands[2].astype(jnp.float32)
        grad_f = operands[3].astype(jnp.float32)
        ids = operands[4]
        allowed = (positions[:, None] >= positions[None, :]) & (ids[:, None] == ids[None, :])
        scores = jnp.einsum('tgd,ud->gtu', query_f, key_f) * score_scale
        scores = jnp.where(allowed, scores, -NEGATIVE)
        row_max = lax.optimization_barrier(jnp.max(scores, -1, keepdims=True))
        shifted = jnp.exp(scores - row_max)
        soft = shifted / lax.optimization_barrier(jnp.sum(shifted, -1, keepdims=True))
        soft_bf = lax.optimization_barrier(soft.astype(jnp.bfloat16)).astype(jnp.float32)
        attended = jnp.einsum('gtu,ud->tgd', soft_bf, value_f)
        row_delta = lax.optimization_barrier(jnp.sum(grad_f * attended, -1))
        dprob = jnp.einsum('tgd,ud->gtu', grad_f, value_f)
        dscore = soft * (dprob - jnp.transpose(row_delta)[:, :, None])
        dscore = lax.optimization_barrier(dscore.astype(jnp.bfloat16)).astype(jnp.float32)
        dquery = (jnp.einsum('gtu,ud->tgd', dscore, key_f) * score_scale).astype(jnp.bfloat16)
        dkey = (jnp.einsum('gtu,tgd->ud', dscore, query_f) * score_scale).astype(jnp.bfloat16)
        dvalue = jnp.einsum('gtu,tgd->ud', soft_bf, grad_f).astype(jnp.bfloat16)
        return (dquery, dkey, dvalue)
    dquery, dkey, dvalue = lax.map(head_grads, (item_queries, item_keys, item_values, item_grads, item_ids))
    dquery = from_items(dquery, (per_kv, HEAD), q_width)
    dkey = from_items(dkey, (HEAD,), kv_width)
    dvalue = from_items(dvalue, (HEAD,), kv_width)
    group_width = q_width // N_MP
    kv_block = kv_width // N_MP
    dq_blocks = dquery.reshape(tokens, N_MP, group_width)
    dkv = jnp.stack([dkey, dvalue], 1).reshape(tokens, 2, N_MP, kv_block)
    dkv_blocks = jnp.transpose(dkv, (0, 2, 1, 3)).reshape(tokens, N_MP, 2 * kv_block)
    grad_blocks = jnp.transpose(jnp.concatenate([dq_blocks, dkv_blocks], 2), (1, 0, 2))
    wq_blocks = w_query.reshape(D, N_MP, group_width)
    wkv_blocks = jnp.transpose(w_keyval.reshape(D, 2, N_MP, kv_block), (0, 2, 1, 3)).reshape(D, N_MP, 2 * kv_block)
    wcat_blocks = jnp.transpose(jnp.concatenate([wq_blocks, wkv_blocks], 2), (1, 2, 0))
    dnormed = block_sum(grad_blocks, wcat_blocks)
    dmerged = (rms_scale * (dnormed - normed_tok * lax.optimization_barrier(jnp.mean(dnormed * normed_tok, -1, keepdims=True)))).astype(jnp.bfloat16)
    dhidden = jnp.dot(dmerged, jnp.transpose(w_merge2), preferred_element_type=jnp.float32)
    dhidden_pre = (dhidden * gelu_grad(hidden_pre)).astype(jnp.bfloat16)
    w1_blocks = jnp.transpose(w_merge1.reshape(4 * V, N_MP, H // N_MP), (1, 2, 0))
    dmerge_in = block_sum(split_rows(dhidden_pre, N_MP), w1_blocks).reshape(tokens * 4, V)
    first_mean = lax.optimization_barrier(jnp.mean(dmerge_in, -1, keepdims=True))
    second_mean = lax.optimization_barrier(jnp.mean(dmerge_in * normed, -1, keepdims=True))
    patch_grad = ln_scale * (dmerge_in - first_mean - normed * second_mean)
    return patch_grad.astype(jnp.bfloat16)
```

```python
import jax
import jax.numpy as jnp
from jax import lax
from jax.sharding import PartitionSpec as P

HEAD = 128


EPSILON = 1e-06
NEGATIVE = 1e30


def shifted_2(value, axis, steps):
    count = lax.axis_size(axis)
    initial, last = (max(0, -steps), min(count, count - steps))
    return lax.ppermute(value, axis, [(source, source + steps) for source in range(initial, last)])


def gelu_grad(inputs):
    normal_cdf = 0.5 * (1.0 + lax.erf(inputs * 0.7071067811865476))
    normal_pdf = jnp.exp(-0.5 * inputs * inputs) * 0.3989422804014327
    return normal_cdf + inputs * normal_pdf


def fetch_earlier(own_keyval, offset):
    return shifted_2(own_keyval, "seq", offset)


def return_terms(terms, offset):
    return (
        shifted_2(terms[0].astype(jnp.bfloat16), "seq", -offset).astype(jnp.float32),
        shifted_2(terms[1].astype(jnp.bfloat16), "seq", -offset).astype(jnp.float32),
    )


def local_gathered(patches, w_merge1, w_merge2, w_query, w_keyval, attn_grad, sample_ids):
    patch_rows, feat_width = patches.shape
    tok_rows = patch_rows // 4
    score_scale = HEAD ** (-0.5)
    values = patches.astype(jnp.float32)
    row_mean = jnp.mean(values, -1, keepdims=True)
    ln_scale = lax.rsqrt(
        jnp.mean(values * values, -1, keepdims=True) - row_mean * row_mean + EPSILON
    )
    normed = (values - row_mean) * ln_scale
    merge_in = normed.astype(jnp.bfloat16).reshape(tok_rows, 4 * feat_width)
    first_tile = lax.all_gather(w_merge1, "seq", axis=1, tiled=True)
    first_flat = first_tile.reshape(4 * feat_width, first_tile.shape[2])
    hidden_pre = jnp.dot(merge_in, first_flat, preferred_element_type=jnp.float32)
    hidden = jax.nn.gelu(hidden_pre, approximate=False).astype(jnp.bfloat16)
    second_tile = lax.all_gather(w_merge2, "seq", axis=1, tiled=True)
    model_width = second_tile.shape[1]
    partial_value = jnp.dot(hidden, second_tile, preferred_element_type=jnp.float32)
    merged = lax.psum(partial_value.astype(jnp.bfloat16), "mp")
    merged_f = merged.astype(jnp.float32)
    rms_scale = lax.rsqrt(jnp.mean(merged_f * merged_f, -1, keepdims=True) + EPSILON)
    normed_tok = merged_f * rms_scale
    query_tile, keyval_tile = (
        lax.all_gather(w_query, "seq", axis=0, tiled=True),
        lax.all_gather(w_keyval, "seq", axis=0, tiled=True),
    )
    kv_part = keyval_tile.shape[2]
    keyval_flat = keyval_tile.reshape(model_width, 2 * kv_part)
    normed_bf = normed_tok.astype(jnp.bfloat16)
    queries = jnp.dot(normed_bf, query_tile, preferred_element_type=jnp.float32).astype(
        jnp.bfloat16
    )
    own_keyval = jnp.dot(normed_bf, keyval_flat, preferred_element_type=jnp.float32).astype(
        jnp.bfloat16
    )
    query_part = queries.shape[1]
    kv_local = kv_part // HEAD
    per_kv = query_part // HEAD // kv_local
    run_ids = sample_ids[0]
    run_len = run_ids.shape[0]
    own_start = lax.axis_index("seq") * tok_rows
    reach = min(lax.axis_size("seq") - 1, (run_len // 2 + 2 * tok_rows - 2) // tok_rows)
    pieces = [own_keyval]
    for offset in range(1, reach + 1):
        pieces.insert(0, fetch_earlier(own_keyval, offset))
    window_kv = jnp.concatenate(pieces, 0)
    window_rows = window_kv.shape[0]
    key_pos = own_start - reach * tok_rows + jnp.arange(window_rows, dtype=jnp.int32)
    padded_ids = jnp.concatenate([jnp.full((reach * tok_rows,), -1, jnp.int32), run_ids], 0)
    key_ids = lax.dynamic_slice_in_dim(padded_ids, own_start, window_rows, 0)
    total_rows = window_kv.shape[0]
    key_heads = window_kv[:, :kv_part].reshape(total_rows, kv_local, HEAD)
    value_heads = window_kv[:, kv_part:].reshape(total_rows, kv_local, HEAD)
    query_pos = own_start + jnp.arange(tok_rows, dtype=jnp.int32)
    own_ids = lax.dynamic_slice_in_dim(run_ids, own_start, tok_rows, 0)
    allowed = (query_pos[:, None] >= key_pos[None, :]) & (own_ids[:, None] == key_ids[None, :])
    query_heads = queries.reshape(tok_rows, kv_local, per_kv, HEAD)
    scores = (
        jnp.einsum("tkgd,ukd->kgtu", query_heads, key_heads, preferred_element_type=jnp.float32)
        * score_scale
    )
    scores = jnp.where(allowed, scores, -NEGATIVE)
    row_max = jnp.max(scores, -1, keepdims=True)
    shifted = jnp.exp(scores - row_max)
    soft = shifted / jnp.sum(shifted, -1, keepdims=True)
    soft_bf = soft.astype(jnp.bfloat16)
    attended = jnp.einsum(
        "kgtu,ukd->tkgd", soft_bf, value_heads, preferred_element_type=jnp.float32
    )
    grad_heads = attn_grad.reshape(tok_rows, kv_local, per_kv, HEAD)
    row_delta = jnp.sum(grad_heads.astype(jnp.float32) * attended, -1)
    dprob = jnp.einsum(
        "tkgd,ukd->kgtu", grad_heads, value_heads, preferred_element_type=jnp.float32
    )
    dscore = (soft * (dprob - jnp.transpose(row_delta, (1, 2, 0))[..., None])).astype(jnp.bfloat16)
    dquery = (
        jnp.einsum("kgtu,ukd->tkgd", dscore, key_heads, preferred_element_type=jnp.float32)
        * score_scale
    )
    dquery = dquery.astype(jnp.bfloat16).reshape(tok_rows, query_part)
    dkey_terms = (
        jnp.einsum("kgtu,tkgd->ukd", dscore, query_heads, preferred_element_type=jnp.float32)
        * score_scale
    )
    dvalue_terms = jnp.einsum(
        "kgtu,tkgd->ukd", soft_bf, grad_heads, preferred_element_type=jnp.float32
    )
    dkey = dkey_terms[reach * tok_rows :]
    dvalue = dvalue_terms[reach * tok_rows :]
    for offset in range(1, reach + 1):
        begin_row = (reach - offset) * tok_rows
        key_back, value_back = return_terms(
            (
                dkey_terms[begin_row : begin_row + tok_rows],
                dvalue_terms[begin_row : begin_row + tok_rows],
            ),
            offset,
        )
        dkey = dkey + key_back
        dvalue = dvalue + value_back
    grads_kv = jnp.concatenate(
        [
            dkey.astype(jnp.bfloat16).reshape(tok_rows, kv_part),
            dvalue.astype(jnp.bfloat16).reshape(tok_rows, kv_part),
        ],
        1,
    )
    dnormed_part = jnp.einsum("tc,dc->td", dquery, query_tile, preferred_element_type=jnp.float32)
    dnormed_part = dnormed_part + jnp.einsum(
        "tc,dc->td", grads_kv, keyval_flat, preferred_element_type=jnp.float32
    )
    dnormed = lax.psum(dnormed_part.astype(jnp.bfloat16), "mp").astype(jnp.float32)
    inner_mean = jnp.mean(dnormed * normed_tok, -1, keepdims=True)
    dmerged = (rms_scale * (dnormed - normed_tok * inner_mean)).astype(jnp.bfloat16)
    dhidden = jnp.einsum("td,hd->th", dmerged, second_tile, preferred_element_type=jnp.float32)
    dhidden_pre = (dhidden * gelu_grad(hidden_pre)).astype(jnp.bfloat16)
    dmerge_part = jnp.einsum(
        "th,fh->tf", dhidden_pre, first_flat, preferred_element_type=jnp.float32
    )
    dmerge_in = lax.psum_scatter(
        dmerge_part.reshape(patch_rows, feat_width).astype(jnp.bfloat16),
        "mp",
        scatter_dimension=0,
        tiled=True,
    ).astype(jnp.float32)
    share_rows = dmerge_in.shape[0]
    begin = lax.axis_index("mp") * share_rows
    own_normed = lax.dynamic_slice_in_dim(normed, begin, share_rows, 0)
    own_scale = lax.dynamic_slice_in_dim(ln_scale, begin, share_rows, 0)
    first_mean = jnp.mean(dmerge_in, -1, keepdims=True)
    second_mean = jnp.mean(dmerge_in * own_normed, -1, keepdims=True)
    patch_grad = own_scale * (dmerge_in - first_mean - own_normed * second_mean)
    return patch_grad.astype(jnp.bfloat16)


def near(value):
    count = lax.axis_size("seq")
    return lax.ppermute(value, "seq", [(s, s ^ 1) for s in range(count)])


def far(value):
    count = lax.axis_size("seq")
    return lax.ppermute(value, "seq", [(s, (s + count // 2) % count) for s in range(count)])


def cross(value):
    return lax.ppermute(value, "mp", [(0, 1), (1, 0)])


def dot(a, b):
    return jnp.dot(a, b, preferred_element_type=jnp.float32)


def dot_t(a, b):
    return lax.dot_general(a, b, (((1,), (1,)), ((), ())), preferred_element_type=jnp.float32)


def pick(array, index, axis):
    return lax.dynamic_index_in_dim(array, index, axis, keepdims=False)


def attention(q, k, v, g, pos, ids):
    score_scale = HEAD ** (-0.5)
    allowed = (pos[:, None] >= pos[None, :]) & (ids[:, None] == ids[None, :])
    scores = (
        jnp.einsum("tkgd,ukd->kgtu", q, k, preferred_element_type=jnp.float32) * score_scale
    )
    scores = jnp.where(allowed, scores, -NEGATIVE)
    row_max = jnp.max(scores, -1, keepdims=True)
    shifted = jnp.exp(scores - row_max)
    soft = shifted / jnp.sum(shifted, -1, keepdims=True)
    soft_bf = soft.astype(jnp.bfloat16)
    dprob = jnp.einsum("tkgd,ukd->kgtu", g, v, preferred_element_type=jnp.float32)
    row_delta = jnp.sum(soft_bf.astype(jnp.float32) * dprob, -1, keepdims=True)
    dscore = (soft * (dprob - row_delta)).astype(jnp.bfloat16)
    dq = jnp.einsum("kgtu,ukd->tkgd", dscore, k, preferred_element_type=jnp.float32) * score_scale
    dk = jnp.einsum("kgtu,tkgd->ukd", dscore, q, preferred_element_type=jnp.float32) * score_scale
    dv = jnp.einsum("kgtu,tkgd->ukd", soft_bf, g, preferred_element_type=jnp.float32)
    return dq.astype(jnp.bfloat16), dk.astype(jnp.bfloat16), dv.astype(jnp.bfloat16)


def local_resident(patches, w_merge1, w_merge2, w_query, w_keyval, attn_grad, sample_ids):
    patch_rows, feat_width = patches.shape
    toks = patch_rows // 4
    seqs = lax.axis_size("seq")
    seq = lax.axis_index("seq")
    mp = lax.axis_index("mp")
    ahead = seq // 2
    core = seq % 2
    feat_part = w_merge1.shape[1]
    hid = w_merge1.shape[2]
    width = w_merge2.shape[1]
    model_width = width * seqs
    rows1 = 4 * feat_part
    q_part = w_query.shape[1]
    kv_part = w_keyval.shape[2]
    q_own = q_part // seqs
    kv_own = kv_part // seqs
    kv_heads = kv_own // HEAD
    per_kv = q_own // kv_own

    w1 = w_merge1.reshape(rows1, hid)
    wkv = w_keyval.reshape(width, 2 * kv_part)
    w1_n = near(w1)
    w2 = w_merge2
    w2_n = near(w2)
    wq = w_query
    wq_n = near(wq)
    wkv_n = near(wkv)

    values = patches.astype(jnp.float32)
    row_mean = jnp.mean(values, -1, keepdims=True)
    ln_scale = lax.rsqrt(
        jnp.mean(values * values, -1, keepdims=True) - row_mean * row_mean + EPSILON
    )
    normed = (values - row_mean) * ln_scale
    pieces = [
        normed[:, j * feat_part : (j + 1) * feat_part].astype(jnp.bfloat16).reshape(toks, rows1)
        for j in range(seqs)
    ]

    def piece(index):
        out = pieces[0]
        for j in range(1, seqs):
            out = jnp.where(index == j, pieces[j], out)
        return out

    x_out = jnp.concatenate([piece(seq ^ 2), piece(seq ^ 3)], 1)
    x_far = far(x_out)
    part_far = dot(x_far[:, :rows1], w1) + dot(x_far[:, rows1:], w1_n)
    back = far(part_far.astype(jnp.bfloat16))
    hidden_pre = dot(piece(seq), w1) + dot(piece(seq ^ 1), w1_n)
    hidden_pre = hidden_pre + back.astype(jnp.float32)
    hidden = jax.nn.gelu(hidden_pre, approximate=False).astype(jnp.bfloat16)

    hidden, attn_grad = lax.optimization_barrier((hidden, attn_grad))
    hidden_far = far(hidden)

    def merged_of(rows):
        mine = [dot(rows, w).astype(jnp.bfloat16) for w in (w2, w2_n)]
        mine = jnp.concatenate(mine, 1)
        return mine, cross(mine)

    def finish(pair):
        total = pair[0].astype(jnp.float32) + pair[1].astype(jnp.float32)
        return total.astype(jnp.bfloat16)

    def columns(q, kv):
        kk, vv = kv[:, :kv_part], kv[:, kv_part:]
        shape = lambda a, w: a.reshape(toks, 2, 2, w)
        return jnp.concatenate([shape(q, q_own), shape(kk, kv_own), shape(vv, kv_own)], -1)

    def project(merged):
        a, b = merged[:, :width], merged[:, width:]
        q = dot(a, wq) + dot(b, wq_n)
        kv = dot(a, wkv) + dot(b, wkv_n)
        cols = columns(q, kv)
        squares = jnp.sum(jnp.square(merged.astype(jnp.float32)), -1, keepdims=True)
        return pick(cols, ahead, 1), far(pick(cols, 1 - ahead, 1).astype(jnp.bfloat16)), squares, far(squares)

    pair_own = merged_of(hidden)
    pair_far = merged_of(hidden_far)
    grads = attn_grad.reshape(toks, 2, 2, q_own)
    grad_far = far(pick(grads, 1 - ahead, 1))
    grad_mine = jnp.stack([pick(grads, ahead, 1), grad_far], 0)
    grad_near = near(pick(grad_mine, 1 - core, 2))
    grad_all = jnp.concatenate([pick(grad_mine, core, 2), grad_near], 0)

    merged_own = finish(pair_own)
    keep_own, got_far, sq_own, sq_own_far = project(merged_own)
    merged_far = finish(pair_far)
    keep_far, got_own, sq_far, sq_far_far = project(merged_far)

    def rms(a, b):
        return lax.rsqrt((a + b) * (1.0 / model_width) + EPSILON)

    rms_own = rms(sq_own, sq_far_far)
    rms_far = rms(sq_far, sq_own_far)
    qkv = jnp.stack(
        [
            ((keep_own + got_own.astype(jnp.float32)) * rms_own[:, :, None]).astype(jnp.bfloat16),
            ((keep_far + got_far.astype(jnp.float32)) * rms_far[:, :, None]).astype(jnp.bfloat16),
        ],
        0,
    )
    qkv_near = near(pick(qkv, 1 - core, 2))
    qkv_all = jnp.concatenate([pick(qkv, core, 2), qkv_near], 0).reshape(seqs * toks, -1)

    run_ids = sample_ids[0].reshape(seqs, toks)
    order = [seq, seq ^ 2, seq ^ 1, seq ^ 3]
    ids = jnp.concatenate([pick(run_ids, o, 0) for o in order], 0)
    pos = jnp.concatenate([o * toks + jnp.arange(toks, dtype=jnp.int32) for o in order], 0)
    rows = seqs * toks
    dq, dk, dv = attention(
        qkv_all[:, :q_own].reshape(rows, kv_heads, per_kv, HEAD),
        qkv_all[:, q_own : q_own + kv_own].reshape(rows, kv_heads, HEAD),
        qkv_all[:, q_own + kv_own :].reshape(rows, kv_heads, HEAD),
        grad_all.reshape(rows, kv_heads, per_kv, HEAD),
        pos,
        ids,
    )
    dall = jnp.concatenate(
        [dq.reshape(rows, q_own), dk.reshape(rows, kv_own), dv.reshape(rows, kv_own)], 1
    )
    dnear = near(dall[2 * toks :])
    dmine = dall[: 2 * toks]
    even = core == 0
    dcols = jnp.stack([jnp.where(even, dmine, dnear), jnp.where(even, dnear, dmine)], 1)
    d_own, d_far = dcols[:toks], dcols[toks:]
    d_far_got = far(d_own)
    d_own_got = far(d_far)

    def natural(mine, other):
        first = ahead == 0
        both = jnp.stack([jnp.where(first, mine, other), jnp.where(first, other, mine)], 1)
        q = both[..., :q_own].reshape(toks, q_part)
        kk = both[..., q_own : q_own + kv_own].reshape(toks, kv_part)
        vv = both[..., q_own + kv_own :].reshape(toks, kv_part)
        return q, jnp.concatenate([kk, vv], 1)

    def dnormed_of(mine, other, merged, scale):
        q, kv = natural(mine, other)
        part = [dot_t(q, a) + dot_t(kv, b) for a, b in ((wq, wkv), (wq_n, wkv_n))]
        part = jnp.concatenate(part, 1).astype(jnp.bfloat16)
        normed_tok = merged.astype(jnp.float32) * scale
        inner = jnp.sum(part.astype(jnp.float32) * normed_tok, -1, keepdims=True)
        return part, cross(part), normed_tok, inner

    parts_far = dnormed_of(d_far, d_far_got, merged_far, rms_far)
    parts_own = dnormed_of(d_own, d_own_got, merged_own, rms_own)
    inner = jnp.stack([parts_own[3], parts_far[3]], 0)
    inner = inner + cross(inner)
    inner = (inner + far(inner)[::-1]) * (1.0 / model_width)

    def dhidden_of(parts, scale, inner):
        part, other, normed_tok, _ = parts
        dnormed = part.astype(jnp.float32) + other.astype(jnp.float32)
        dmerged = (scale * (dnormed - normed_tok * inner)).astype(jnp.bfloat16)
        return dot_t(dmerged[:, :width], w2) + dot_t(dmerged[:, width:], w2_n)

    dh_far = far(dhidden_of(parts_far, rms_far, inner[1]).astype(jnp.bfloat16))
    dhidden = dhidden_of(parts_own, rms_own, inner[0]) + dh_far.astype(jnp.float32)
    dhidden_pre = (dhidden * gelu_grad(hidden_pre)).astype(jnp.bfloat16)
    dpre_far = far(dhidden_pre)
    dpre = jnp.stack([dhidden_pre, dpre_far], 0).reshape(2 * toks, hid)
    dparts = jnp.stack([dot_t(dpre, w1), dot_t(dpre, w1_n)], 1).astype(jnp.bfloat16)
    share = toks // 2
    dparts = dparts.reshape(2, 2, share, 2, rows1)
    dsum = pick(dparts, mp, 1).astype(jnp.float32) + cross(pick(dparts, 1 - mp, 1)).astype(
        jnp.float32
    )
    dother = far(dsum[1].astype(jnp.bfloat16)).astype(jnp.float32)
    dsum = dsum[0]
    blocks = [dsum[:, 0], dsum[:, 1], dother[:, 0], dother[:, 1]]
    blocks = [b.reshape(share * 4, feat_part) for b in blocks]

    def block(index):
        out = blocks[0]
        for j in range(1, seqs):
            out = jnp.where((seq ^ index) == j, blocks[j], out)
        return out

    dmerge_in = jnp.concatenate([block(j) for j in range(seqs)], 1)
    share_rows = dmerge_in.shape[0]
    begin = mp * share_rows
    own_normed = lax.dynamic_slice_in_dim(normed, begin, share_rows, 0)
    own_scale = lax.dynamic_slice_in_dim(ln_scale, begin, share_rows, 0)
    first_mean = jnp.mean(dmerge_in, -1, keepdims=True)
    second_mean = jnp.mean(dmerge_in * own_normed, -1, keepdims=True)
    patch_grad = own_scale * (dmerge_in - first_mean - own_normed * second_mean)
    return patch_grad.astype(jnp.bfloat16)


def local(patches, w_merge1, w_merge2, w_query, w_keyval, attn_grad, sample_ids):
    seqs = lax.axis_size("seq")
    kv_heads = w_keyval.shape[2] // HEAD
    plan = local_gathered
    if seqs == 4 and lax.axis_size("mp") == 2 and kv_heads % seqs == 0:
        plan = local_resident
    return plan(patches, w_merge1, w_merge2, w_query, w_keyval, attn_grad, sample_ids)


def solution(mesh):
    in_specs = (
        P(("group", "seq"), None),
        P(None, "seq", "mp"),
        P("mp", "seq"),
        P("seq", "mp"),
        P("seq", None, "mp"),
        P(("group", "seq"), "mp"),
        P("group", None),
    )
    out_specs = P(("group", "seq", "mp"), None)
    return jax.shard_map(local, mesh=mesh, in_specs=in_specs, out_specs=out_specs, check_vma=False)
```

```python
import jax
import jax.numpy as jnp
from jax import lax
from jax.experimental import pallas as pl
from jax.experimental.pallas import tpu as pltpu
from jax.sharding import PartitionSpec as P

HEAD = 128


EPSILON = 1e-06
NEGATIVE = 1e30


def shifted_2(value, axis, steps):
    count = lax.axis_size(axis)
    initial, last = (max(0, -steps), min(count, count - steps))
    return lax.ppermute(value, axis, [(source, source + steps) for source in range(initial, last)])


def gelu_grad(inputs):
    normal_cdf = 0.5 * (1.0 + lax.erf(inputs * 0.7071067811865476))
    normal_pdf = jnp.exp(-0.5 * inputs * inputs) * 0.3989422804014327
    return normal_cdf + inputs * normal_pdf


def fetch_earlier(own_keyval, offset):
    return shifted_2(own_keyval, "seq", offset)


def return_terms(terms, offset):
    return (
        shifted_2(terms[0].astype(jnp.bfloat16), "seq", -offset).astype(jnp.float32),
        shifted_2(terms[1].astype(jnp.bfloat16), "seq", -offset).astype(jnp.float32),
    )


def local_gathered(patches, w_merge1, w_merge2, w_query, w_keyval, attn_grad, sample_ids):
    patch_rows, feat_width = patches.shape
    tok_rows = patch_rows // 4
    score_scale = HEAD ** (-0.5)
    values = patches.astype(jnp.float32)
    row_mean = jnp.mean(values, -1, keepdims=True)
    ln_scale = lax.rsqrt(
        jnp.mean(values * values, -1, keepdims=True) - row_mean * row_mean + EPSILON
    )
    normed = (values - row_mean) * ln_scale
    merge_in = normed.astype(jnp.bfloat16).reshape(tok_rows, 4 * feat_width)
    first_tile = lax.all_gather(w_merge1, "seq", axis=1, tiled=True)
    first_flat = first_tile.reshape(4 * feat_width, first_tile.shape[2])
    hidden_pre = jnp.dot(merge_in, first_flat, preferred_element_type=jnp.float32)
    hidden = jax.nn.gelu(hidden_pre, approximate=False).astype(jnp.bfloat16)
    second_tile = lax.all_gather(w_merge2, "seq", axis=1, tiled=True)
    model_width = second_tile.shape[1]
    partial_value = jnp.dot(hidden, second_tile, preferred_element_type=jnp.float32)
    merged = lax.psum(partial_value.astype(jnp.bfloat16), "mp")
    merged_f = merged.astype(jnp.float32)
    rms_scale = lax.rsqrt(jnp.mean(merged_f * merged_f, -1, keepdims=True) + EPSILON)
    normed_tok = merged_f * rms_scale
    query_tile, keyval_tile = (
        lax.all_gather(w_query, "seq", axis=0, tiled=True),
        lax.all_gather(w_keyval, "seq", axis=0, tiled=True),
    )
    kv_part = keyval_tile.shape[2]
    keyval_flat = keyval_tile.reshape(model_width, 2 * kv_part)
    normed_bf = normed_tok.astype(jnp.bfloat16)
    queries = jnp.dot(normed_bf, query_tile, preferred_element_type=jnp.float32).astype(
        jnp.bfloat16
    )
    own_keyval = jnp.dot(normed_bf, keyval_flat, preferred_element_type=jnp.float32).astype(
        jnp.bfloat16
    )
    query_part = queries.shape[1]
    kv_local = kv_part // HEAD
    per_kv = query_part // HEAD // kv_local
    run_ids = sample_ids[0]
    run_len = run_ids.shape[0]
    own_start = lax.axis_index("seq") * tok_rows
    reach = min(lax.axis_size("seq") - 1, (run_len // 2 + 2 * tok_rows - 2) // tok_rows)
    pieces = [own_keyval]
    for offset in range(1, reach + 1):
        pieces.insert(0, fetch_earlier(own_keyval, offset))
    window_kv = jnp.concatenate(pieces, 0)
    window_rows = window_kv.shape[0]
    key_pos = own_start - reach * tok_rows + jnp.arange(window_rows, dtype=jnp.int32)
    padded_ids = jnp.concatenate([jnp.full((reach * tok_rows,), -1, jnp.int32), run_ids], 0)
    key_ids = lax.dynamic_slice_in_dim(padded_ids, own_start, window_rows, 0)
    total_rows = window_kv.shape[0]
    key_heads = window_kv[:, :kv_part].reshape(total_rows, kv_local, HEAD)
    value_heads = window_kv[:, kv_part:].reshape(total_rows, kv_local, HEAD)
    query_pos = own_start + jnp.arange(tok_rows, dtype=jnp.int32)
    own_ids = lax.dynamic_slice_in_dim(run_ids, own_start, tok_rows, 0)
    allowed = (query_pos[:, None] >= key_pos[None, :]) & (own_ids[:, None] == key_ids[None, :])
    query_heads = queries.reshape(tok_rows, kv_local, per_kv, HEAD)
    scores = (
        jnp.einsum("tkgd,ukd->kgtu", query_heads, key_heads, preferred_element_type=jnp.float32)
        * score_scale
    )
    scores = jnp.where(allowed, scores, -NEGATIVE)
    row_max = jnp.max(scores, -1, keepdims=True)
    shifted = jnp.exp(scores - row_max)
    soft = shifted / jnp.sum(shifted, -1, keepdims=True)
    soft_bf = soft.astype(jnp.bfloat16)
    attended = jnp.einsum(
        "kgtu,ukd->tkgd", soft_bf, value_heads, preferred_element_type=jnp.float32
    )
    grad_heads = attn_grad.reshape(tok_rows, kv_local, per_kv, HEAD)
    row_delta = jnp.sum(grad_heads.astype(jnp.float32) * attended, -1)
    dprob = jnp.einsum(
        "tkgd,ukd->kgtu", grad_heads, value_heads, preferred_element_type=jnp.float32
    )
    dscore = (soft * (dprob - jnp.transpose(row_delta, (1, 2, 0))[..., None])).astype(jnp.bfloat16)
    dquery = (
        jnp.einsum("kgtu,ukd->tkgd", dscore, key_heads, preferred_element_type=jnp.float32)
        * score_scale
    )
    dquery = dquery.astype(jnp.bfloat16).reshape(tok_rows, query_part)
    dkey_terms = (
        jnp.einsum("kgtu,tkgd->ukd", dscore, query_heads, preferred_element_type=jnp.float32)
        * score_scale
    )
    dvalue_terms = jnp.einsum(
        "kgtu,tkgd->ukd", soft_bf, grad_heads, preferred_element_type=jnp.float32
    )
    dkey = dkey_terms[reach * tok_rows :]
    dvalue = dvalue_terms[reach * tok_rows :]
    for offset in range(1, reach + 1):
        begin_row = (reach - offset) * tok_rows
        key_back, value_back = return_terms(
            (
                dkey_terms[begin_row : begin_row + tok_rows],
                dvalue_terms[begin_row : begin_row + tok_rows],
            ),
            offset,
        )
        dkey = dkey + key_back
        dvalue = dvalue + value_back
    grads_kv = jnp.concatenate(
        [
            dkey.astype(jnp.bfloat16).reshape(tok_rows, kv_part),
            dvalue.astype(jnp.bfloat16).reshape(tok_rows, kv_part),
        ],
        1,
    )
    dnormed_part = jnp.einsum("tc,dc->td", dquery, query_tile, preferred_element_type=jnp.float32)
    dnormed_part = dnormed_part + jnp.einsum(
        "tc,dc->td", grads_kv, keyval_flat, preferred_element_type=jnp.float32
    )
    dnormed = lax.psum(dnormed_part.astype(jnp.bfloat16), "mp").astype(jnp.float32)
    inner_mean = jnp.mean(dnormed * normed_tok, -1, keepdims=True)
    dmerged = (rms_scale * (dnormed - normed_tok * inner_mean)).astype(jnp.bfloat16)
    dhidden = jnp.einsum("td,hd->th", dmerged, second_tile, preferred_element_type=jnp.float32)
    dhidden_pre = (dhidden * gelu_grad(hidden_pre)).astype(jnp.bfloat16)
    dmerge_part = jnp.einsum(
        "th,fh->tf", dhidden_pre, first_flat, preferred_element_type=jnp.float32
    )
    dmerge_in = lax.psum_scatter(
        dmerge_part.reshape(patch_rows, feat_width).astype(jnp.bfloat16),
        "mp",
        scatter_dimension=0,
        tiled=True,
    ).astype(jnp.float32)
    share_rows = dmerge_in.shape[0]
    begin = lax.axis_index("mp") * share_rows
    own_normed = lax.dynamic_slice_in_dim(normed, begin, share_rows, 0)
    own_scale = lax.dynamic_slice_in_dim(ln_scale, begin, share_rows, 0)
    first_mean = jnp.mean(dmerge_in, -1, keepdims=True)
    second_mean = jnp.mean(dmerge_in * own_normed, -1, keepdims=True)
    patch_grad = own_scale * (dmerge_in - first_mean - own_normed * second_mean)
    return patch_grad.astype(jnp.bfloat16)


BF16 = jnp.bfloat16
F32 = jnp.float32
LANES = 128


def near(value):
    count = lax.axis_size("seq")
    return lax.ppermute(value, "seq", [(s, s ^ 1) for s in range(count)])


def far(value):
    count = lax.axis_size("seq")
    return lax.ppermute(value, "seq", [(s, (s + count // 2) % count) for s in range(count)])


def cross(value):
    return lax.ppermute(value, "mp", [(0, 1), (1, 0)])


def dot(a, b):
    return jnp.dot(a, b, preferred_element_type=F32)


def dot_t(a, b):
    return lax.dot_general(a, b, (((1,), (1,)), ((), ())), preferred_element_type=F32)


def dot_l(a, b):
    return lax.dot_general(a, b, (((0,), (0,)), ((), ())), preferred_element_type=F32)


def struct(shape, dtype):
    return jax.ShapeDtypeStruct(shape, dtype)


def whole(shape):
    return pl.BlockSpec(shape, lambda *_: (0,) * len(shape))


def call(body, name, grid, ins, outs, scratch, meta, *operands):
    return pl.pallas_call(
        body,
        grid_spec=pltpu.PrefetchScalarGridSpec(
            num_scalar_prefetch=1,
            grid=grid,
            in_specs=ins,
            out_specs=[spec for spec, _ in outs],
            scratch_shapes=scratch,
        ),
        out_shape=[shape for _, shape in outs],
        compiler_params=pltpu.CompilerParams(
            dimension_semantics=("arbitrary",) * len(grid), vmem_limit_bytes=48 << 20
        ),
        name=name,
    )(meta, *operands)


def full(shape, dtype):
    return whole(shape), struct(shape, dtype)


def layer_norm(values):
    row_mean = jnp.mean(values, -1, keepdims=True)
    scale = lax.rsqrt(jnp.mean(values * values, -1, keepdims=True) - row_mean * row_mean + EPSILON)
    return (values - row_mean) * scale, scale


def prepare(meta, patches, seqs):
    rows, feats = patches.shape
    toks, part = rows // 4, feats // seqs
    tiles = feats // LANES

    def body(meta, x, own, other, buf):
        seq = meta[0] // 2
        normed = layer_norm(x[...].astype(F32))[0]
        for n in range(tiles):
            buf[n] = normed[:, n * LANES : (n + 1) * LANES]
        lanes = [
            jnp.concatenate([buf[n, pl.ds(p, toks, stride=4), :] for n in range(tiles)], 1)
            for p in range(4)
        ]
        for j in range(seqs):
            cols = [v[:, j * part : (j + 1) * part] for v in lanes]
            cols = jnp.concatenate(cols, 1).astype(BF16)
            place = seq ^ j
            for r in range(2):

                @pl.when(place == r)
                def _():
                    own[r] = cols

                @pl.when(place == r + 2)
                def _():
                    other[r] = cols

    shape = (2, toks, 4 * part)
    return call(
        body, "prepare", (1,), [whole(patches.shape)], [full(shape, BF16)] * 2,
        [pltpu.VMEM((tiles, rows, LANES), F32)], meta, patches,
    )


def first(meta, x, w, w_n, dtype):
    _, toks, depth = x.shape
    hid = w.shape[1]
    bn = hid // 2

    def body(_, x, w, w_n, out):
        out[...] = (dot(x[0], w[...]) + dot(x[1], w_n[...])).astype(dtype)

    col = pl.BlockSpec((depth, bn), lambda n, _: (0, n))
    return call(
        body, "first", (hid // bn,), [whole(x.shape), col, col],
        [(pl.BlockSpec((toks, bn), lambda n, _: (0, n)), struct((toks, hid), dtype))], [],
        meta, x, w, w_n,
    )[0]


def merge_hidden(meta, part, back, w, w_n):
    toks, hid = part.shape
    width = w.shape[1]
    bn = width // 4

    def body(_, part, back, w, w_n, pre, hidden, out):
        @pl.when(pl.program_id(0) == 0)
        def _():
            total = part[...] + back[...].astype(F32)
            pre[...] = total
            hidden[...] = (total * 0.5 * (1.0 + lax.erf(total * 0.7071067811865476))).astype(BF16)

        rows = hidden[...]
        out[0] = dot(rows, w[...]).astype(BF16)
        out[1] = dot(rows, w_n[...]).astype(BF16)

    col = pl.BlockSpec((hid, bn), lambda n, _: (0, n))
    return call(
        body, "merge_hidden", (width // bn,), [whole(part.shape), whole(part.shape), col, col],
        [full(part.shape, F32), full(part.shape, BF16),
         (pl.BlockSpec((2, toks, bn), lambda n, _: (0, 0, n)), struct((2, toks, width), BF16))],
        [], meta, part, back, w, w_n,
    )


def merge_far(meta, hidden, w, w_n):
    toks, hid = hidden.shape
    width = w.shape[1]
    bn = width // 4

    def body(_, hidden, w, w_n, out):
        out[0] = dot(hidden[...], w[...]).astype(BF16)
        out[1] = dot(hidden[...], w_n[...]).astype(BF16)

    col = pl.BlockSpec((hid, bn), lambda n, _: (0, n))
    return call(
        body, "merge_far", (width // bn,), [whole(hidden.shape), col, col],
        [(pl.BlockSpec((2, toks, bn), lambda n, _: (0, 0, n)), struct((2, toks, width), BF16))],
        [], meta, hidden, w, w_n,
    )[0]


def column_specs(weights, swap):
    wq, _, wkv, _ = weights
    width = wq.shape[0]
    q_own, kv_own = wq.shape[1] // 4, wkv.shape[1] // 8

    def place(c, meta):
        return ((meta[0] // 2) ^ (2 * swap)) ^ c

    q = pl.BlockSpec((width, q_own), lambda c, meta: (0, place(c, meta)))
    k = pl.BlockSpec((width, kv_own), lambda c, meta: (0, place(c, meta)))
    v = pl.BlockSpec((width, kv_own), lambda c, meta: (0, 4 + place(c, meta)))
    operands = [wq, weights[1], wkv, weights[3], wkv, weights[3]]
    return [q, q, k, k, v, v], operands, q_own, kv_own


def project_send(meta, mine, other, weights):
    _, toks, width = mine.shape
    specs, operands, q_own, kv_own = column_specs(weights, 1)
    cols = q_own + 2 * kv_own

    def body(_, mine, other, q, qn, k, kn, v, vn, merged, squares, out):
        @pl.when(pl.program_id(0) == 0)
        def _():
            total = (mine[...].astype(F32) + other[...].astype(F32)).astype(BF16)
            merged[...] = total
            wide = total.astype(F32)
            squares[...] = jnp.sum(jnp.sum(wide * wide, 0), -1, keepdims=True)

        a, b = merged[0], merged[1]
        out[0, :, :q_own] = (dot(a, q[...]) + dot(b, qn[...])).astype(BF16)
        out[0, :, q_own : q_own + kv_own] = (dot(a, k[...]) + dot(b, kn[...])).astype(BF16)
        out[0, :, q_own + kv_own :] = (dot(a, v[...]) + dot(b, vn[...])).astype(BF16)

    return call(
        body, "project_send", (2,), [whole(mine.shape)] * 2 + specs,
        [full(mine.shape, BF16), full((toks, 1), F32),
         (pl.BlockSpec((1, toks, cols), lambda c, _: (c, 0, 0)), struct((2, toks, cols), BF16))],
        [], meta, mine, other, *operands,
    )


def project_keep(meta, merged, weights):
    _, toks, width = merged.shape
    specs, operands, q_own, kv_own = column_specs(weights, 0)
    cols = q_own + 2 * kv_own

    def body(_, merged, q, qn, k, kn, v, vn, out):
        a, b = merged[0], merged[1]
        out[0, :, :q_own] = dot(a, q[...]) + dot(b, qn[...])
        out[0, :, q_own : q_own + kv_own] = dot(a, k[...]) + dot(b, kn[...])
        out[0, :, q_own + kv_own :] = dot(a, v[...]) + dot(b, vn[...])

    return call(
        body, "project_keep", (2,), [whole(merged.shape)] + specs,
        [(pl.BlockSpec((1, toks, cols), lambda c, _: (c, 0, 0)), struct((2, toks, cols), F32))],
        [], meta, merged, *operands,
    )[0]


def scale_heads(meta, keeps, gots, rms):
    _, toks, cols = gots[0].shape

    def body(_, k0, k1, g0, g1, rms, mine, side):
        for i, (k, g) in enumerate(((k0, g0), (k1, g1))):
            total = (k[...] + g[...].astype(F32)) * rms[i][None]
            mine[i] = total[0].astype(BF16)
            side[i] = total[1].astype(BF16)

    return call(
        body, "scale_heads", (1,), [whole(gots[0].shape)] * 4 + [whole(rms.shape)],
        [full((2, toks, cols), BF16)] * 2, [], meta, *keeps, *gots, rms,
    )


def attention(meta, mine, side, grad_mine, grad_side, ids_row, ids_col):
    _, toks, cols = mine.shape
    q_own = grad_mine.shape[2]
    kv_own = (cols - q_own) // 2
    heads, per_kv = kv_own // HEAD, q_own // kv_own
    scale = HEAD ** (-0.5)
    tiles = 4
    lanes = per_kv * toks

    def body(meta, mine, side, g_mine, g_side, ids_row, ids_col, d_own, d_far, d_side, dk_buf, dv_buf):
        seq = meta[0] // 2
        order = [seq, seq ^ 2, seq ^ 1, seq ^ 3]
        qkv = [mine.at[0], mine.at[1], side.at[0], side.at[1]]
        grads = [g_mine.at[0], g_mine.at[1], g_side.at[0], g_side.at[1]]
        outs = [d_own, d_far, d_side.at[0], d_side.at[1]]
        key_pos = jnp.concatenate(
            [o * toks + lax.broadcasted_iota(jnp.int32, (toks, 1), 0) for o in order], 0
        )
        key_ids = jnp.concatenate([ids_col[o] for o in order], 0)
        for h in range(heads):
            ks = slice(q_own + h * HEAD, q_own + (h + 1) * HEAD)
            vs = slice(q_own + kv_own + h * HEAD, q_own + kv_own + (h + 1) * HEAD)
            keys = jnp.concatenate([r[:, ks] for r in qkv], 0)
            vals = jnp.concatenate([r[:, vs] for r in qkv], 0)
            for i in range(tiles):
                qs = [slice((h * per_kv + g) * HEAD, (h * per_kv + g + 1) * HEAD) for g in range(per_kv)]
                q = jnp.concatenate([qkv[i][:, s] for s in qs], 0)
                g = jnp.concatenate([grads[i][:, s] for s in qs], 0)
                pos = order[i] * toks + lax.broadcasted_iota(jnp.int32, (1, toks), 1)
                allowed = (pos >= key_pos) & (ids_row[order[i]] == key_ids)
                allowed = jnp.concatenate([allowed] * per_kv, 1)
                s = jnp.where(allowed, dot_t(keys, q) * scale, -NEGATIVE)
                e = jnp.exp(s - jnp.max(s, 0, keepdims=True))
                soft = e / jnp.sum(e, 0, keepdims=True)
                soft_bf = soft.astype(BF16)
                dprob = dot_t(vals, g)
                delta = jnp.sum(soft_bf.astype(F32) * dprob, 0, keepdims=True)
                ds = (soft * (dprob - delta)).astype(BF16)
                dk, dv = dot(ds, q), dot(soft_bf, g)
                if i == 0:
                    dk_buf[...], dv_buf[...] = dk, dv
                else:
                    dk_buf[...] += dk
                    dv_buf[...] += dv
                dq = (dot_l(ds, keys) * scale).astype(BF16)
                for n, s_ in enumerate(qs):
                    outs[i][:, s_] = dq[n * toks : (n + 1) * toks]
            for i in range(tiles):
                outs[i][:, ks] = (dk_buf[i * toks : (i + 1) * toks] * scale).astype(BF16)
                outs[i][:, vs] = dv_buf[i * toks : (i + 1) * toks].astype(BF16)

    shape = (toks, cols)
    return call(
        body, "attention", (1,),
        [whole(a.shape) for a in (mine, side, grad_mine, grad_side, ids_row, ids_col)],
        [full(shape, BF16), full(shape, BF16), full((2,) + shape, BF16)],
        [pltpu.VMEM((tiles * toks, HEAD), F32)] * 2,
        meta, mine, side, grad_mine, grad_side, ids_row, ids_col,
    )


def spread(a, q, k, v, q_own, kv_own):
    return (
        dot_t(a[:, :q_own], q[...])
        + dot_t(a[:, q_own : q_own + kv_own], k[...])
        + dot_t(a[:, q_own + kv_own :], v[...])
    )


def dnormed_mine(meta, d_own, d_far, d_side, weights):
    toks, cols = d_own.shape
    specs, operands, q_own, kv_own = column_specs(weights, 0)
    width = weights[0].shape[0]

    def body(_, own, other, side, q, qn, k, kn, v, vn, acc):
        @pl.when(pl.program_id(0) == 0)
        def _():
            a = jnp.concatenate([own[...], other[...]], 0)
            acc[:, :width] = spread(a, q, k, v, q_own, kv_own)
            acc[:, width:] = spread(a, qn, kn, vn, q_own, kv_own)

        @pl.when(pl.program_id(0) == 1)
        def _():
            a = side[...].reshape(2 * toks, cols)
            acc[:, :width] += spread(a, q, k, v, q_own, kv_own)
            acc[:, width:] += spread(a, qn, kn, vn, q_own, kv_own)

    return call(
        body, "dnormed_mine", (2,),
        [whole(d_own.shape)] * 2 + [whole(d_side.shape)] + specs,
        [full((2 * toks, 2 * width), F32)], [], meta, d_own, d_far, d_side, *operands,
    )[0]


def dnormed_rest(meta, acc, chunk, got, got_side, merged, rms, weights):
    toks, cols = got.shape
    specs, operands, q_own, kv_own = column_specs(weights, 1)
    width = weights[0].shape[0]

    def body(_, acc, got, got_side, merged, rms, q, qn, k, kn, v, vn, out, inner, buf):
        @pl.when(pl.program_id(0) == 0)
        def _():
            a = got[...]
            buf[0] = acc[:, :width] + spread(a, q, k, v, q_own, kv_own)
            buf[1] = acc[:, width:] + spread(a, qn, kn, vn, q_own, kv_own)

        @pl.when(pl.program_id(0) == 1)
        def _():
            a = got_side[...]
            total = jnp.zeros((toks, 1), F32)
            for i, (x, y, z) in enumerate(((q, k, v), (qn, kn, vn))):
                part = (buf[i] + spread(a, x, y, z, q_own, kv_own)).astype(BF16)
                out[i] = part
                total += jnp.sum(part.astype(F32) * merged[i].astype(F32), -1, keepdims=True)
            inner[...] = total * rms[...]

    return call(
        body, "dnormed_rest", (2,),
        [pl.BlockSpec((toks, 2 * width), lambda c, _: (chunk, 0)), whole(got.shape),
         whole(got.shape), whole(merged.shape), whole(rms.shape)] + specs,
        [full((2, toks, width), BF16), full((toks, 1), F32)],
        [pltpu.VMEM((2, toks, width), F32)],
        meta, acc, got, got_side, merged, rms, *operands,
    )


def dhidden_of(meta, part, other, merged, rms, inner, w, w_n, tail=None):
    _, toks, width = part.shape
    hid = w.shape[0]
    bn = hid // 5 if hid % 640 == 0 else hid

    def body(_, part, other, merged, rms, inner, w, w_n, *rest):
        out, buf = rest[-2:]

        @pl.when(pl.program_id(0) == 0)
        def _():
            dnormed = part[...].astype(F32) + other[...].astype(F32)
            normed = merged[...].astype(F32) * rms[...][None]
            buf[...] = (rms[...][None] * (dnormed - normed * inner[...][None])).astype(BF16)

        total = dot_t(buf[0], w[...]) + dot_t(buf[1], w_n[...])
        if tail is not None:
            back, pre = rest[:2]
            total = (total + back[...].astype(F32)) * gelu_grad(pre[...])
        out[...] = total.astype(BF16)

    row = pl.BlockSpec((bn, width), lambda n, _: (n, 0))
    col = pl.BlockSpec((toks, bn), lambda n, _: (0, n))
    return call(
        body, "dhidden", (hid // bn,),
        [whole(part.shape)] * 3 + [whole(rms.shape)] * 2 + [row, row] + [col] * len(tail or ()),
        [(col, struct((toks, hid), BF16))], [pltpu.VMEM(part.shape, BF16)],
        meta, part, other, merged, rms, inner, w, w_n, *(tail or ()),
    )[0]


def dmerge(meta, d_own, d_far, w, w_n):
    toks, hid = d_own.shape
    depth = w.shape[0]
    half = toks // 2
    bn = depth // 5 if depth % 640 == 0 else depth

    def body(meta, own, other, w, w_n, send, keep):
        mp = meta[0] % 2
        for out, start in ((send, (1 - mp) * half), (keep, mp * half)):
            rows = pl.ds(pl.multiple_of(start, half), half)
            a = jnp.concatenate([own[rows, :], other[rows, :]], 0)
            out[0] = dot_t(a, w[...]).astype(out.dtype)
            out[1] = dot_t(a, w_n[...]).astype(out.dtype)

    row = pl.BlockSpec((bn, hid), lambda n, _: (n, 0))
    col = pl.BlockSpec((2, toks, bn), lambda n, _: (0, 0, n))
    return call(
        body, "dmerge", (depth // bn,), [whole(d_own.shape)] * 2 + [row, row],
        [(col, struct((2, toks, depth), BF16)), (col, struct((2, toks, depth), BF16))], [],
        meta, d_own, d_far, w, w_n,
    )


def finish(meta, keep, got, other, patches, seqs):
    rows, feats = patches.shape
    share = rows // 2
    toks = share // 4
    part = feats // seqs
    tiles = feats // LANES

    def body(meta, keep, got, other, x, out, blocks, buf):
        seq = meta[0] // 2
        for r in range(2):
            blocks[r] = keep[r, :toks].astype(F32) + got[r, :toks].astype(F32)
            blocks[r + 2] = other[r].astype(F32)
        cols = [blocks[seq ^ j] for j in range(seqs)]
        for p in range(4):
            row = jnp.concatenate([c[:, p * part : (p + 1) * part] for c in cols], 1)
            for n in range(tiles):
                buf[n, pl.ds(p, toks, stride=4), :] = row[:, n * LANES : (n + 1) * LANES]
        grad = jnp.concatenate([buf[n] for n in range(tiles)], 1)
        normed, scale = layer_norm(x[...].astype(F32))
        first_mean = jnp.mean(grad, -1, keepdims=True)
        second_mean = jnp.mean(grad * normed, -1, keepdims=True)
        out[...] = (scale * (grad - first_mean - normed * second_mean)).astype(BF16)

    return call(
        body, "finish", (1,),
        [whole(keep.shape), whole(got.shape), whole(other.shape),
         pl.BlockSpec((share, feats), lambda _, meta: (meta[0] % 2, 0))],
        [full((share, feats), BF16)],
        [pltpu.VMEM((seqs, toks, 4 * part), F32), pltpu.VMEM((tiles, share, LANES), F32)],
        meta, keep, got, other, patches,
    )[0]


def local_resident(patches, w_merge1, w_merge2, w_query, w_keyval, attn_grad, sample_ids):
    patch_rows, feat_width = patches.shape
    toks = patch_rows // 4
    seqs = lax.axis_size("seq")
    seq = lax.axis_index("seq")
    meta = jnp.full((1,), seq * 2 + lax.axis_index("mp"), jnp.int32)
    hid = w_merge1.shape[2]
    width = w_merge2.shape[1]
    model_width = width * seqs
    q_own = w_query.shape[1] // seqs

    w1 = w_merge1.reshape(-1, hid)
    wkv = w_keyval.reshape(width, -1)
    w1_n = near(w1)
    x_own, x_out = prepare(meta, patches, seqs)
    x_far = far(x_out)
    w2 = w_merge2
    w2_n = near(w2)
    weights = (w_query, near(w_query), wkv, near(wkv))

    part_own = first(meta, x_own, w1, w1_n, F32)
    part_far = first(meta, x_far, w1, w1_n, BF16)
    back = far(part_far)
    hidden_pre, hidden, mine_own = merge_hidden(meta, part_own, back, w2, w2_n)
    hidden_far = far(hidden)
    other_own = cross(mine_own)
    mine_far = merge_far(meta, hidden_far, w2, w2_n)
    other_far = cross(mine_far)

    mine_own, attn_grad = lax.optimization_barrier((mine_own, attn_grad))
    ahead, core = seq // 2, seq % 2
    grads = attn_grad.reshape(toks, 2, 2, q_own)

    def pick(array, index, axis):
        return lax.dynamic_index_in_dim(array, index, axis, keepdims=False)

    grads = jnp.transpose(grads, (1, 2, 0, 3))
    grads_keep = pick(grads, ahead, 0)
    grads_got = far(pick(grads, 1 - ahead, 0))
    grad_mine = jnp.stack([pick(grads_keep, core, 0), pick(grads_got, core, 0)], 0)
    grad_side = near(jnp.stack([pick(grads_keep, 1 - core, 0), pick(grads_got, 1 - core, 0)], 0))

    merged_own, sq_own, send_own = project_send(meta, mine_own, other_own, weights)
    got_far = far(send_own)
    keep_own = project_keep(meta, merged_own, weights)
    merged_far, sq_far, send_far = project_send(meta, mine_far, other_far, weights)
    got_own = far(send_far)
    squares = jnp.stack([sq_own, sq_far], 0)
    squares_got = far(squares)
    keep_far = project_keep(meta, merged_far, weights)
    rms = lax.rsqrt((squares + squares_got[::-1]) * (1.0 / model_width) + EPSILON)
    qkv_mine, qkv_out = scale_heads(meta, (keep_own, keep_far), (got_own, got_far), rms)
    qkv_side = near(qkv_out)

    run_ids = sample_ids.reshape(seqs, toks)
    d_own, d_far, d_out = attention(
        meta, qkv_mine, qkv_side, grad_mine, grad_side, run_ids[:, None, :], run_ids[:, :, None]
    )
    d_far_got = far(d_own)
    d_own_got = far(d_far)
    d_side = near(d_out)
    d_far_got_side = far(d_side[0])
    d_own_got_side = far(d_side[1])
    acc = dnormed_mine(meta, d_own, d_far, d_side, weights)
    dn_far, in_far = dnormed_rest(
        meta, acc, 1, d_far_got, d_far_got_side, merged_far, rms[1], weights
    )
    dn_far_got = cross(dn_far)
    dn_own, in_own = dnormed_rest(
        meta, acc, 0, d_own_got, d_own_got_side, merged_own, rms[0], weights
    )
    dn_own_got = cross(dn_own)
    inner = jnp.stack([in_own, in_far], 0)
    inner = inner + cross(inner)
    inner = (inner + far(inner)[::-1]) * (1.0 / model_width)
    dh_far = dhidden_of(meta, dn_far, dn_far_got, merged_far, rms[1], inner[1], w2, w2_n)
    dh_back = far(dh_far)
    dpre_own = dhidden_of(
        meta, dn_own, dn_own_got, merged_own, rms[0], inner[0], w2, w2_n, (dh_back, hidden_pre)
    )
    dpre_far = far(dpre_own)
    send, keep = dmerge(meta, dpre_own, dpre_far, w1, w1_n)
    got = cross(send)
    half = toks // 2
    other = (keep[:, half:].astype(F32) + got[:, half:].astype(F32)).astype(BF16)
    return finish(meta, keep, got, far(other), patches, seqs)


def local(patches, w_merge1, w_merge2, w_query, w_keyval, attn_grad, sample_ids):
    seqs = lax.axis_size("seq")
    kv_heads = w_keyval.shape[2] // HEAD
    plan = local_gathered
    if seqs == 4 and lax.axis_size("mp") == 2 and kv_heads % seqs == 0:
        plan = local_resident
    return plan(patches, w_merge1, w_merge2, w_query, w_keyval, attn_grad, sample_ids)


def solution(mesh):
    in_specs = (
        P(("group", "seq"), None),
        P(None, "seq", "mp"),
        P("mp", "seq"),
        P("seq", "mp"),
        P("seq", None, "mp"),
        P(("group", "seq"), "mp"),
        P("group", None),
    )
    out_specs = P(("group", "seq", "mp"), None)
    return jax.shard_map(local, mesh=mesh, in_specs=in_specs, out_specs=out_specs, check_vma=False)
```
